32 devices in a mesh: section: 4 (over y, core), expert: 2 (over x), tensor: 4 (over z).
Axes of the slice: x: 2, y: 2, z: 4, core: 2. Of those that a mesh axis runs over, the one named last changes fastest.
Arguments:
- branch_weights: bfloat16 [2, 8192, 8192], P('expert', ('section', 'tensor')), may hold values from -0.125 to 0.125
- branch_gains: float32 [2, 8192], P('expert', ('section', 'tensor')), may hold values from 0.1 to 1.9
- column_order: int32 [2, 8192], P('expert'), may hold values from 0 to 8191, each once within a row
- layer_order: int32 [4], replicated, may hold values from 0 to 3, each once
- probe_seeds: int32 [1024], replicated, may hold values from 1 to 32767
Outputs:
- expert_weights: bfloat16 [2, 8192, 8192], P('expert', None, ('section', 'tensor'))
- checksum: float32 [2, 1024, 8192], P('expert', None, ('section', 'tensor'))
- fingerprint: float32 [2, 1024], P('expert')
- shared_gain: float32 [8192], replicated
The draws below stay inside these ranges and needn't reach their ends.
Inputs may be any that keep to these rules, and one draw needn't show every extreme that they name: Each row of column_order names every hidden unit once. layer_order names every layer once.
All inputs are finite; a program needn't handle non-finite values.
Results may differ from the reference program's by a relative error of at most 0.0034.
Values may be sent and summed in bfloat16 or wider, within the bound.
A program may use at most 64 MiB of HBM per device.

```python
import jax
import jax.numpy as jnp
from jax import lax

D = 2048
FF = 8192
LAYERS = 4
PROBES = 1024
EXPERTS = 2


def touch_ends(drawn, rng, least, top_value):
    index_at = [jax.random.randint(jax.random.fold_in(rng, axis), (), 0, length) for axis, length in enumerate(drawn.shape)]
    main_axis = drawn.shape.index(max(drawn.shape))
    beside = index_at[:main_axis] + [(index_at[main_axis] + 1) % drawn.shape[main_axis]] + index_at[main_axis + 1:]
    return drawn.at[tuple(index_at)].set(least).at[tuple(beside)].set(top_value)


def steps_of(key, shape, shards, least, top_value):
    factor_of = 1.0
    for dim, parts in shards:
        heights = jax.random.uniform(jax.random.fold_in(jax.random.fold_in(key, 6), dim), (parts,), jnp.float32, least / len(shards), top_value / len(shards))
        factor_of = factor_of * jnp.repeat(jnp.exp(heights), shape[dim] // parts).reshape((-1,) + (1,) * (len(shape) - 1 - dim))
    return factor_of


def scatter_about(key, dims, width, bound, split=(), kind=jnp.bfloat16):
    entries = width * jax.random.normal(key, dims, jnp.float32)
    if split:
        entries = entries * steps_of(key, dims, split, -0.22, 0.18)
    return jnp.clip(entries, -bound, bound).astype(kind)


def setup_inputs(seed: int = 0) -> dict:
    key_of = jax.random.split(jax.random.key(seed), 6)
    return {
        "branch_weights": scatter_about(key_of[0], (EXPERTS, LAYERS * D, FF), D ** -0.5, 0.125, ((0, 2), (1, 16))),
        "branch_gains": jnp.clip(1.0 + 0.18 * jax.random.normal(key_of[1], (EXPERTS, LAYERS * D), jnp.float32), 0.1, 1.9),
        "column_order": jax.vmap(lambda own: jax.random.permutation(own, FF))(jax.random.split(key_of[2], EXPERTS)).reshape((EXPERTS, FF)).astype(jnp.int32),
        "layer_order": jax.random.permutation(key_of[3], LAYERS).astype(jnp.int32),
        "probe_seeds": touch_ends(jax.random.randint(key_of[4], (PROBES,), 1, 32768), jax.random.fold_in(key_of[4], 1), 1, 32767).astype(jnp.int32),
    }


def probe_at(probe_seeds, row_ids):
    hashed = (probe_seeds[:, None] * (row_ids[None, :] + 1)) % 65521
    return ((hashed % 511) - 255).astype(jnp.float32) / 256.0


def reference(branch_weights, branch_gains, column_order, layer_order, probe_seeds):
    mean_gain = jnp.sum(branch_gains, axis=0) / EXPERTS
    slot_ids = jnp.arange(LAYERS, dtype=jnp.int32)
    inverse = jnp.sum(jnp.where(layer_order[None, :] == slot_ids[:, None], slot_ids[None, :], 0), axis=1).astype(jnp.int32)
    shared_gain = mean_gain.reshape(LAYERS, D)[inverse].reshape(LAYERS * D)
    probes = probe_at(probe_seeds, jnp.arange(LAYERS * D, dtype=jnp.int32)).astype(jnp.bfloat16)
    seven = jnp.full((1,), 7919, jnp.int32)
    column_probe = probe_at(seven, jnp.arange(FF, dtype=jnp.int32))[0]

    def one_expert(inputs):
        weights, own_gains, order = inputs
        permuted = jnp.take(weights, order, axis=1)
        scaling = own_gains / mean_gain
        folded = (permuted.astype(jnp.float32) * scaling[:, None]).astype(jnp.bfloat16)
        natural = folded.reshape(LAYERS, D, FF)[inverse].reshape(LAYERS * D, FF)
        sketches = jnp.dot(probes, natural, preferred_element_type=jnp.float32)
        printed = jnp.dot(sketches, column_probe, precision=lax.Precision.HIGHEST) * (FF ** -0.5)
        return natural, sketches, printed

    expert_weights, checksum, fingerprint = lax.map(one_expert, (branch_weights, branch_gains, column_order))
    return expert_weights, checksum, fingerprint, shared_gain
```

```python
import functools

import jax
import jax.numpy as jnp
from jax import lax
from jax.experimental import pallas as pl
from jax.experimental.pallas import tpu as pltpu
from jax.sharding import PartitionSpec as P

MESH = pl.DeviceIdType.MESH


def probe_values(products):
    folded = (products >> 16) * 15 + (products & 65535)
    hashed = jnp.where(folded >= 65521, folded - 65521, folded)
    digits = (hashed >> 9) + (hashed & 511)
    digits = jnp.where(digits >= 511, digits - 511, digits)
    return (digits - 255).astype(jnp.float32) * (1.0 / 256.0)


def exchange(
    n_section, n_expert, n_tensor, layers,
    order_s, w_hbm, gains_ref, cols_ref, seeds_ref,
    arrived_hbm, sums_ref, print_ref, means_ref,
    w, staged, arrived, acc, onehot, scale, print_acc, seed_col, probes, gains, parts,
    w_sem, send_sem, recv_sem, out_sem, gain_send, gain_recv, mean_send, mean_recv,
    part_send, part_recv,
):
    section, expert, tensor = (lax.axis_index(a) for a in ("section", "expert", "tensor"))
    groups = n_section * n_tensor
    me = section * n_tensor + tensor
    rows, width = w.shape
    cols = width // groups
    n_probes = seed_col.shape[0]
    deep = onehot.shape[0]
    n_deep = width // deep
    per_layer = groups // layers
    half = n_tensor // 2 if n_tensor % 2 == 0 else n_tensor
    sides = n_tensor // half

    def partner(k, sign):
        m, cross = k // sides, (k + 1) % sides
        j, i = (m + 1) % half, (m // half + 1) % n_section
        t = ((tensor // half + cross) % sides) * half + (tensor % half + sign * j + half) % half
        return (section + sign * i + n_section) % n_section, t

    def remote(src, dst, send, recv, k):
        s, t = partner(k, 1)
        return pltpu.make_async_remote_copy(
            src_ref=src, dst_ref=dst, send_sem=send.at[k], recv_sem=recv.at[k],
            device_id={"section": s, "tensor": t}, device_id_type=MESH)

    def block_copy(k):
        s, t = partner(k, 1)
        return remote(staged.at[s * n_tensor + t], arrived.at[me], send_sem, recv_sem, k)

    def mean_copy(k):
        return remote(means_ref.at[me], means_ref.at[me], mean_send, mean_recv, k)

    def part_copy(k):
        return remote(parts.at[me], parts.at[me], part_send, part_recv, k)

    def gain_copy(j):
        return pltpu.make_async_remote_copy(
            src_ref=gains_ref, dst_ref=gains.at[expert], send_sem=gain_send.at[j],
            recv_sem=gain_recv.at[j], device_id={"expert": (expert + j + 1) % n_expert},
            device_id_type=MESH)

    def w_copy(c):
        at = pl.ds(pl.multiple_of(c * deep, deep), deep)
        return pltpu.make_async_copy(w_hbm.at[0, :, at], w.at[:, at], w_sem.at[c])

    def out_copy(k, g):
        return pltpu.make_async_copy(arrived.at[g], arrived_hbm.at[g], out_sem.at[k])

    @pl.loop(0, n_deep)
    def _(c):
        w_copy(c).start()

    barrier = pltpu.get_barrier_semaphore()

    @pl.loop(0, groups - 1)
    def _(k):
        s, t = partner(k, 1)
        pl.semaphore_signal(
            barrier, inc=1, device_id={"section": s, "tensor": t}, device_id_type=MESH)

    @pl.loop(0, n_expert - 1)
    def _(j):
        pl.semaphore_signal(
            barrier, inc=1, device_id={"expert": (expert + j + 1) % n_expert},
            device_id_type=MESH)

    print_acc[...] = jnp.zeros_like(print_acc)
    sums_ref[...] = jnp.zeros_like(sums_ref)
    seeds = seeds_ref[...]
    seed_col[...] = jnp.broadcast_to(
        seeds.astype(jnp.float32), (128, n_probes)).T.astype(jnp.int32)
    pl.semaphore_wait(barrier, groups - 1 + n_expert - 1)

    @pl.loop(0, n_expert - 1)
    def _(j):
        gain_copy(j).start()

    own = gains_ref[...]
    gains[expert] = own

    @pl.loop(0, n_expert - 1)
    def _(j):
        gain_copy(j).wait()

    total = gains[0]
    for e in range(1, n_expert):
        total = total + gains[e]
    mean = total / n_expert
    means_ref[me] = mean
    scale[...] = jnp.broadcast_to(own / mean, (128, rows)).T

    @pl.loop(0, groups - 1)
    def _(k):
        mean_copy(k).start()

    @pl.loop(0, groups)
    def _(k):
        s, t = partner(k, 1)
        g = s * n_tensor + t
        at = pl.ds(pl.multiple_of(g * cols, cols), cols)
        wanted = cols_ref[:, at]
        acc[...] = jnp.zeros_like(acc)

        @pl.loop(0, n_deep)
        def _(c):
            @pl.when(k == 0)
            def _():
                w_copy(c).wait()

            ids = lax.broadcasted_iota(jnp.int32, (deep, cols), 0)
            onehot[...] = jnp.where(ids == wanted - c * deep, 1.0, 0.0).astype(jnp.bfloat16)
            acc[...] += jnp.dot(
                w[:, pl.ds(pl.multiple_of(c * deep, deep), deep)], onehot[...],
                preferred_element_type=jnp.float32)

        column_ids = g * cols + lax.broadcasted_iota(jnp.int32, (1, cols), 1)
        column_probe = probe_values(7919 * (column_ids + 1))
        for c in range(cols // 128):
            part = slice(c * 128, (c + 1) * 128)
            block = (acc[:, part] * scale[...]).astype(jnp.bfloat16)
            staged[g, :, part] = block
            print_acc[...] += block.astype(jnp.float32) * column_probe[:, part]

        @pl.when(k < groups - 1)
        def _():
            block_copy(k).start()

    def first_row(g):
        return order_s[g // per_layer] * (rows * per_layer) + (g % per_layer) * rows

    totals = jnp.sum(print_acc[...], axis=1, keepdims=True)
    row_ids = first_row(me) + lax.broadcasted_iota(jnp.int32, (rows, 128), 0)
    for c in range(n_probes // 128):
        part = slice(c * 128, (c + 1) * 128)
        values = probe_values(seeds[:, part] * (row_ids + 1))
        parts[me, :, part] = jnp.sum(values * totals, axis=0, keepdims=True)

    @pl.loop(0, groups - 1)
    def _(k):
        part_copy(k).start()

    def sketch(k, block):
        s, t = partner(k, -1)
        g = s * n_tensor + t
        first = first_row(g) + 1
        chunk = min(64, n_probes)

        @pl.loop(0, n_probes // chunk)
        def _(r):
            at = pl.ds(pl.multiple_of(r * chunk, chunk), chunk)
            for c in range(rows // 128):
                ids = first + c * 128 + lax.broadcasted_iota(jnp.int32, (1, 128), 1)
                probes[at, c * 128:(c + 1) * 128] = probe_values(
                    seed_col[at, :] * ids).astype(jnp.bfloat16)

        sums_ref[...] += jnp.dot(probes[...], block, preferred_element_type=jnp.float32)

    arrived[me] = staged[me]
    out_copy(groups - 1, me).start()
    sketch(groups - 1, staged[me])

    @pl.loop(0, groups - 1)
    def _(k):
        s, t = partner(k, -1)
        g = s * n_tensor + t
        block_copy(k).wait_recv()
        out_copy(k, g).start()
        sketch(k, arrived[g])

    @pl.loop(0, groups - 1)
    def _(k):
        part_copy(k).wait()
        mean_copy(k).wait()

    printed = parts[0]
    for g in range(1, groups):
        printed = printed + parts[g]
    print_ref[...] = printed * width ** -0.5

    @pl.loop(0, groups - 1)
    def _(k):
        s, t = partner(k, -1)
        block_copy(k).wait_send()
        out_copy(k, s * n_tensor + t).wait()

    out_copy(groups - 1, me).wait()


def place(order_s, blocks_ref, sums_ref, print_ref, means_ref,
          weights_out, sums_out, print_out, means_out):
    weights_out[...] = blocks_ref[...]
    sums_out[...] = sums_ref[...]
    print_out[...] = print_ref[...]
    means_out[...] = means_ref[...]


def local(n_section, n_expert, n_tensor, branch_weights, branch_gains, column_order,
          layer_order, probe_seeds):
    _, rows, width = branch_weights.shape
    groups = n_section * n_tensor
    cols = width // groups
    layers = layer_order.shape[0]
    n_probes = probe_seeds.shape[0]
    per_layer = groups // layers
    deep = min(1024, width)
    f32, bf16 = jnp.float32, jnp.bfloat16
    vmem = pl.BlockSpec(memory_space=pltpu.VMEM)
    hbm = pl.BlockSpec(memory_space=pl.ANY)
    dma = pltpu.SemaphoreType.DMA
    arrived, sums, printed, means = pl.pallas_call(
        functools.partial(exchange, n_section, n_expert, n_tensor, layers),
        out_shape=(
            jax.ShapeDtypeStruct((groups, rows, cols), bf16),
            jax.ShapeDtypeStruct((n_probes, cols), f32),
            jax.ShapeDtypeStruct((1, n_probes), f32),
            jax.ShapeDtypeStruct((groups, 1, rows), f32),
        ),
        in_specs=[pl.BlockSpec(memory_space=pltpu.SMEM), hbm, vmem, vmem, vmem],
        out_specs=(hbm, vmem, vmem, vmem),
        scratch_shapes=[
            pltpu.VMEM((rows, width), bf16),
            pltpu.VMEM((groups, rows, cols), bf16),
            pltpu.VMEM((groups, rows, cols), bf16),
            pltpu.VMEM((rows, cols), f32),
            pltpu.VMEM((deep, cols), bf16),
            pltpu.VMEM((rows, 128), f32),
            pltpu.VMEM((rows, 128), f32),
            pltpu.VMEM((n_probes, 128), jnp.int32),
            pltpu.VMEM((n_probes, rows), bf16),
            pltpu.VMEM((n_expert, 1, rows), f32),
            pltpu.VMEM((groups, 1, n_probes), f32),
            dma((width // deep,)), dma((groups,)), dma((groups,)), dma((groups,)),
            dma((n_expert,)), dma((n_expert,)), dma((groups,)), dma((groups,)),
            dma((groups,)), dma((groups,)),
        ],
        compiler_params=pltpu.CompilerParams(
            collective_id=0, has_side_effects=True, vmem_limit_bytes=56 * 2 ** 20),
        name="exchange",
    )(layer_order, branch_weights, branch_gains, column_order, probe_seeds.reshape(1, n_probes))

    def placed(g, order):
        return (order[g // per_layer] * per_layer + g % per_layer, 0, 0)

    share = n_probes // groups
    weights, sums, printed, means = pl.pallas_call(
        place,
        grid_spec=pltpu.PrefetchScalarGridSpec(
            num_scalar_prefetch=1,
            grid=(groups,),
            in_specs=[
                pl.BlockSpec((1, rows, cols), lambda g, order: (g, 0, 0)),
                pl.BlockSpec((share, cols), lambda g, order: (g, 0)),
                pl.BlockSpec((1, n_probes), lambda g, order: (0, 0)),
                pl.BlockSpec((1, 1, rows), lambda g, order: (g, 0, 0)),
            ],
            out_specs=[
                pl.BlockSpec((1, rows, cols), placed),
                pl.BlockSpec((share, cols), lambda g, order: (g, 0)),
                pl.BlockSpec((1, n_probes), lambda g, order: (0, 0)),
                pl.BlockSpec((1, 1, rows), placed),
            ],
        ),
        out_shape=(
            jax.ShapeDtypeStruct((groups, rows, cols), bf16),
            jax.ShapeDtypeStruct((n_probes, cols), f32),
            jax.ShapeDtypeStruct((1, n_probes), f32),
            jax.ShapeDtypeStruct((groups, 1, rows), f32),
        ),
        name="place",
    )(layer_order, arrived, sums, printed, means)
    return (weights.reshape(1, groups * rows, cols), sums[None], printed,
            means.reshape(groups * rows))


def solution(mesh):
    sizes = mesh.shape
    return jax.shard_map(
        functools.partial(local, sizes["section"], sizes["expert"], sizes["tensor"]),
        mesh=mesh,
        in_specs=(
            P("expert", ("section", "tensor"), None),
            P("expert", ("section", "tensor")),
            P("expert", None),
            P(),
            P(),
        ),
        out_specs=(
            P("expert", None, ("section", "tensor")),
            P("expert", None, ("section", "tensor")),
            P("expert", None),
            P(),
        ),
        check_vma=False,
    )
```

```python
import functools

import jax
import jax.numpy as jnp
from jax import lax
from jax.experimental import pallas as pl
from jax.experimental.pallas import tpu as pltpu
from jax.sharding import PartitionSpec as P

MESH = pl.DeviceIdType.MESH


def probe_values(products):
    folded = (products >> 16) * 15 + (products & 65535)
    hashed = jnp.where(folded >= 65521, folded - 65521, folded)
    digits = (hashed >> 9) + (hashed & 511)
    digits = jnp.where(digits >= 511, digits - 511, digits)
    return (digits - 255).astype(jnp.float32) * (1.0 / 256.0)


def exchange(
    n_section, n_expert, n_tensor, layers,
    order_s, w_hbm, gains_ref, cols_ref, seeds_ref,
    arrived, sums_ref, print_ref, means_ref,
    w, staged, acc, onehot, scale, print_acc, seed_col, probes, gains, parts,
    w_sem, send_sem, recv_sem, gain_send, gain_recv, mean_send, mean_recv,
    part_send, part_recv,
):
    section, expert, tensor = (lax.axis_index(a) for a in ("section", "expert", "tensor"))
    groups = n_section * n_tensor
    me = section * n_tensor + tensor
    rows, width = w.shape
    cols = width // groups
    n_probes = seed_col.shape[0]
    deep = onehot.shape[0]
    n_deep = width // deep
    per_layer = groups // layers
    half = n_tensor // 2 if n_tensor % 2 == 0 else n_tensor
    sides = n_tensor // half

    def partner(k, sign):
        m, cross = k // sides, (k + 1) % sides
        j = cross * (m // n_section % half) + (1 - cross) * ((m + 1) % half)
        q = cross * (m % n_section) + (1 - cross) * ((m + 1) // half % n_section)
        i = q if n_section % 2 else q % 2 * (n_section // 2) + q // 2
        t = ((tensor // half + cross) % sides) * half + (tensor % half + sign * j + half) % half
        return (section + sign * i + n_section) % n_section, t

    def remote(src, dst, send, recv, k):
        s, t = partner(k, 1)
        return pltpu.make_async_remote_copy(
            src_ref=src, dst_ref=dst, send_sem=send.at[k], recv_sem=recv.at[k],
            device_id={"section": s, "tensor": t}, device_id_type=MESH)

    def block_copy(k):
        s, t = partner(k, 1)
        return remote(staged.at[s * n_tensor + t], arrived.at[me], send_sem, recv_sem, k)

    def mean_copy(k):
        return remote(means_ref.at[me], means_ref.at[me], mean_send, mean_recv, k)

    def part_copy(k):
        return remote(parts.at[me], parts.at[me], part_send, part_recv, k)

    def gain_copy(j):
        return pltpu.make_async_remote_copy(
            src_ref=gains_ref, dst_ref=gains.at[expert], send_sem=gain_send.at[j],
            recv_sem=gain_recv.at[j], device_id={"expert": (expert + j + 1) % n_expert},
            device_id_type=MESH)

    def w_copy(c):
        at = pl.ds(pl.multiple_of(c * deep, deep), deep)
        return pltpu.make_async_copy(w_hbm.at[0, :, at], w.at[:, at], w_sem.at[c])

    @pl.loop(0, n_deep)
    def _(c):
        w_copy(c).start()

    barrier = pltpu.get_barrier_semaphore()

    @pl.loop(0, groups - 1)
    def _(k):
        s, t = partner(k, 1)
        pl.semaphore_signal(
            barrier, inc=1, device_id={"section": s, "tensor": t}, device_id_type=MESH)

    @pl.loop(0, n_expert - 1)
    def _(j):
        pl.semaphore_signal(
            barrier, inc=1, device_id={"expert": (expert + j + 1) % n_expert},
            device_id_type=MESH)

    print_acc[...] = jnp.zeros_like(print_acc)
    pl.semaphore_wait(barrier, groups - 1 + n_expert - 1)

    @pl.loop(0, n_expert - 1)
    def _(j):
        gain_copy(j).start()

    @pl.loop(0, groups)
    def _(k):
        s, t = partner(k, 1)
        g = s * n_tensor + t
        at = pl.ds(pl.multiple_of(g * cols, cols), cols)
        wanted = cols_ref[:, at]
        acc[...] = jnp.zeros_like(acc)

        @pl.loop(0, n_deep)
        def _(c):
            @pl.when(k == 0)
            def _():
                w_copy(c).wait()

            ids = lax.broadcasted_iota(jnp.int32, (deep, cols), 0)
            onehot[...] = jnp.where(ids == wanted - c * deep, 1.0, 0.0).astype(jnp.bfloat16)
            acc[...] += jnp.dot(
                w[:, pl.ds(pl.multiple_of(c * deep, deep), deep)], onehot[...],
                preferred_element_type=jnp.float32)

        @pl.when(k == 0)
        def _():
            own = gains_ref[...]
            gains[expert] = own

            @pl.loop(0, n_expert - 1)
            def _(j):
                gain_copy(j).wait()

            total = gains[0]
            for e in range(1, n_expert):
                total = total + gains[e]
            mean = total / n_expert
            means_ref[me] = mean
            scale[...] = jnp.broadcast_to(own / mean, (128, rows)).T

        column_ids = g * cols + lax.broadcasted_iota(jnp.int32, (1, cols), 1)
        column_probe = probe_values(7919 * (column_ids + 1))
        for c in range(cols // 128):
            part = slice(c * 128, (c + 1) * 128)
            block = (acc[:, part] * scale[...]).astype(jnp.bfloat16)
            staged[g, :, part] = block
            print_acc[...] += block.astype(jnp.float32) * column_probe[:, part]

        @pl.when(k < groups - 1)
        def _():
            block_copy(k).start()

    @pl.loop(0, groups - 1)
    def _(k):
        mean_copy(k).start()

    sums_ref[...] = jnp.zeros_like(sums_ref)
    seeds = seeds_ref[...]
    seed_col[...] = jnp.broadcast_to(
        seeds.astype(jnp.float32), (128, n_probes)).T.astype(jnp.int32)

    def first_row(g):
        return order_s[g // per_layer] * (rows * per_layer) + (g % per_layer) * rows

    totals = jnp.sum(print_acc[...], axis=1, keepdims=True)
    row_ids = first_row(me) + lax.broadcasted_iota(jnp.int32, (rows, 128), 0)
    for c in range(n_probes // 128):
        part = slice(c * 128, (c + 1) * 128)
        values = probe_values(seeds[:, part] * (row_ids + 1))
        parts[me, :, part] = jnp.sum(values * totals, axis=0, keepdims=True)

    @pl.loop(0, groups - 1)
    def _(k):
        part_copy(k).start()

    def sketch(k, block):
        s, t = partner(k, -1)
        g = s * n_tensor + t
        first = first_row(g) + 1
        chunk = min(64, n_probes)

        @pl.loop(0, n_probes // chunk)
        def _(r):
            at = pl.ds(pl.multiple_of(r * chunk, chunk), chunk)
            for c in range(rows // 128):
                ids = first + c * 128 + lax.broadcasted_iota(jnp.int32, (1, 128), 1)
                probes[at, c * 128:(c + 1) * 128] = probe_values(
                    seed_col[at, :] * ids).astype(jnp.bfloat16)

        sums_ref[...] += jnp.dot(probes[...], block, preferred_element_type=jnp.float32)

    arrived[me] = staged[me]
    sketch(groups - 1, staged[me])

    @pl.loop(0, groups - 1)
    def _(k):
        s, t = partner(k, -1)
        g = s * n_tensor + t
        block_copy(k).wait_recv()
        sketch(k, arrived[g])

    @pl.loop(0, groups - 1)
    def _(k):
        part_copy(k).wait()
        mean_copy(k).wait()

    printed = parts[0]
    for g in range(1, groups):
        printed = printed + parts[g]
    print_ref[...] = printed * width ** -0.5

    @pl.loop(0, groups - 1)
    def _(k):
        block_copy(k).wait_send()


def place(order_s, blocks_ref, sums_ref, print_ref, means_ref,
          weights_out, sums_out, print_out, means_out, block_sem, mean_sem, flat_sem):
    groups = blocks_ref.shape[0]
    per_layer = groups // order_s.shape[0]

    def copies(g):
        to = order_s[g // per_layer] * per_layer + g % per_layer
        return (pltpu.make_async_copy(blocks_ref.at[g], weights_out.at[to], block_sem.at[g]),
                pltpu.make_async_copy(means_ref.at[g], means_out.at[to], mean_sem.at[g]))

    flat = (pltpu.make_async_copy(sums_ref, sums_out, flat_sem.at[0]),
            pltpu.make_async_copy(print_ref, print_out, flat_sem.at[1]))

    @pl.loop(0, groups)
    def _(g):
        for copy in copies(g):
            copy.start()

    for copy in flat:
        copy.start()

    @pl.loop(0, groups)
    def _(g):
        for copy in copies(g):
            copy.wait()

    for copy in flat:
        copy.wait()


def local(n_section, n_expert, n_tensor, branch_weights, branch_gains, column_order,
          layer_order, probe_seeds):
    _, rows, width = branch_weights.shape
    groups = n_section * n_tensor
    cols = width // groups
    layers = layer_order.shape[0]
    n_probes = probe_seeds.shape[0]
    per_layer = groups // layers
    deep = min(1024, width)
    f32, bf16 = jnp.float32, jnp.bfloat16
    vmem = pl.BlockSpec(memory_space=pltpu.VMEM)
    hbm = pl.BlockSpec(memory_space=pl.ANY)
    dma = pltpu.SemaphoreType.DMA
    arrived, sums, printed, means = pl.pallas_call(
        functools.partial(exchange, n_section, n_expert, n_tensor, layers),
        out_shape=(
            jax.ShapeDtypeStruct((groups, rows, cols), bf16),
            jax.ShapeDtypeStruct((n_probes, cols), f32),
            jax.ShapeDtypeStruct((1, n_probes), f32),
            jax.ShapeDtypeStruct((groups, 1, rows), f32),
        ),
        in_specs=[pl.BlockSpec(memory_space=pltpu.SMEM), hbm, vmem, vmem, vmem],
        out_specs=(vmem, vmem, vmem, vmem),
        scratch_shapes=[
            pltpu.VMEM((rows, width), bf16),
            pltpu.VMEM((groups, rows, cols), bf16),
            pltpu.VMEM((rows, cols), f32),
            pltpu.VMEM((deep, cols), bf16),
            pltpu.VMEM((rows, 128), f32),
            pltpu.VMEM((rows, 128), f32),
            pltpu.VMEM((n_probes, 128), jnp.int32),
            pltpu.VMEM((n_probes, rows), bf16),
            pltpu.VMEM((n_expert, 1, rows), f32),
            pltpu.VMEM((groups, 1, n_probes), f32),
            dma((width // deep,)), dma((groups,)), dma((groups,)),
            dma((n_expert,)), dma((n_expert,)), dma((groups,)), dma((groups,)),
            dma((groups,)), dma((groups,)),
        ],
        compiler_params=pltpu.CompilerParams(
            collective_id=0, has_side_effects=True, vmem_limit_bytes=40 * 2 ** 20),
        name="exchange",
    )(layer_order, branch_weights, branch_gains, column_order, probe_seeds.reshape(1, n_probes))

    weights, sums, printed, means = pl.pallas_call(
        place,
        in_specs=[pl.BlockSpec(memory_space=pltpu.SMEM), vmem, vmem, vmem, vmem],
        out_specs=(hbm, hbm, hbm, hbm),
        scratch_shapes=[dma((groups,)), dma((groups,)), dma((2,))],
        out_shape=(
            jax.ShapeDtypeStruct((groups, rows, cols), bf16),
            jax.ShapeDtypeStruct((n_probes, cols), f32),
            jax.ShapeDtypeStruct((1, n_probes), f32),
            jax.ShapeDtypeStruct((groups, 1, rows), f32),
        ),
        compiler_params=pltpu.CompilerParams(
            has_side_effects=True, vmem_limit_bytes=16 * 2 ** 20),
        name="place",
    )(layer_order, arrived, sums, printed, means)
    return (weights.reshape(1, groups * rows, cols), sums[None], printed,
            means.reshape(groups * rows))


def solution(mesh):
    sizes = mesh.shape
    return jax.shard_map(
        functools.partial(local, sizes["section"], sizes["expert"], sizes["tensor"]),
        mesh=mesh,
        in_specs=(
            P("expert", ("section", "tensor"), None),
            P("expert", ("section", "tensor")),
            P("expert", None),
            P(),
            P(),
        ),
        out_specs=(
            P("expert", None, ("section", "tensor")),
            P("expert", None, ("section", "tensor")),
            P("expert", None),
            P(),
        ),
        check_vma=False,
    )
```
